768 devices in a mesh: dp: 24 (over z_hi, y), seq: 16 (over z_lo, x), mp: 2 (over core).
Axes of the slice: x: 4, y: 8, z: 12 (z_hi: 3, z_lo: 4; z = z_hi * 4 + z_lo), core: 2. Of those that a mesh axis runs over, the one named last changes fastest.
Arguments:
- features: bfloat16 [24, 32, 32, 16, 256], P('dp', 'seq'), may hold values from -6 to 6
- conv_weight: bfloat16 [3, 3, 3, 256, 256], replicated, may hold values from -0.078125 to 0.078125
- latent_weight: bfloat16 [256, 16], replicated, may hold values from -0.375 to 0.375
- order: int32 [256], replicated, may hold values from 0 to 255, each once
- embed_weight: bfloat16 [64, 6144], P(None, 'mp'), may hold values from -0.75 to 0.75
- cotangent: bfloat16 [98304, 6144], P(('dp', 'seq'), 'mp'), may hold values from -0.078125 to 0.078125
Outputs:
- embedded: bfloat16 [98304, 6144], P(('dp', 'seq'), 'mp')
- embed_grad: float32 [2, 64, 3072], P('mp', None, ('dp', 'seq'))
The draws below stay inside these ranges and needn't reach their ends.
Inputs may be any that keep to these rules, and one draw needn't show every extreme that they name: order is a permutation of the positions of a band.
All inputs are finite; a program needn't handle non-finite values.
Results may differ from the reference program's by a relative error of at most 0.0058.
Values may be sent and summed in bfloat16 or wider, within the bound.
A program may use at most 32 MiB of HBM per device.

```python
import jax
import jax.numpy as jnp
from jax import lax

CH = 256
LAT = 16
D = 6144
WW = 16
PIN = 64
HH = 32
FRAMES = 32
CLIPS = 24
TOK_DEV = 256
TOKENS = 98304
N_SEQ = 16
N_MP = 2


def raised(result, key, source, target, blocks, factor):
    owner, partner = [(jnp.arange(result.shape[position]) // (result.shape[position] // blocks)).reshape([-1 if axis == position else 1 for axis in range(result.ndim)]) for position in (source, target)]
    chosen = jax.random.permutation(key, blocks)[partner]
    strong = (owner == chosen) | (owner == (partner + blocks // 2) % blocks)
    return jnp.where(strong, factor * result, result)


def shard_levels(rng, dims, cuts, low, top_value):
    factor_of, own = 1.0, jax.random.fold_in(rng, 6)
    for dim, parts in cuts:
        steps = jnp.exp(jax.random.uniform(jax.random.fold_in(own, dim), (parts,), jnp.float32, low / len(cuts), top_value / len(cuts)))
        factor_of = factor_of * jnp.repeat(steps, dims[dim] // parts).reshape([-1 if axis == dim else 1 for axis in range(len(dims))])
    return factor_of


def noise(own_key, shape, spread, most, shards=(), held_as=jnp.bfloat16):
    result = jax.random.normal(own_key, shape, jnp.float32) * spread
    if len(shards) > 0:
        result = shard_levels(own_key, shape, shards, -0.22, 0.18) * result
    return jnp.clip(result, min=-most, max=most).astype(held_as)


def bell_draw_with(key, extent, spread, most, split, heavy, kind=jnp.bfloat16):
    values = spread * jax.random.normal(key, extent, jnp.float32)
    if split:
        values = values * shard_levels(key, extent, split, -0.22, 0.18)
    return jnp.clip(raised(values, jax.random.fold_in(key, 3), *heavy), -most, most).astype(kind)


def setup_inputs(seed: int = 0) -> dict:
    keys = jax.random.split(jax.random.key(seed), 7)
    return {
        "features": noise(keys[0], (CLIPS, FRAMES, HH, WW, CH), 1.0, 6.0, ((0, 24), (1, 16))),
        "conv_weight": noise(keys[1], (3, 3, 3, CH, CH), (27 * CH) ** -0.5, 0.078125),
        "latent_weight": noise(keys[2], (CH, LAT), CH ** -0.5, 0.375),
        "order": jax.random.permutation(keys[3], TOK_DEV).astype(jnp.int32),
        "embed_weight": noise(keys[4], (PIN, D), PIN ** -0.5, 0.75, ((1, 2),)),
        "cotangent": bell_draw_with(keys[5], (TOKENS, D), (TOKENS ** -0.5), 0.078125, ((0, 384), (1, 2)), (0, 1, 384, 6.0)),
    }


def reference(features, conv_weight, latent_weight, order, embed_weight, cotangent):
    conv = lax.conv_general_dilated(features, conv_weight, (1, 1, 1), ((2, 0), (1, 1), (1, 1)), dimension_numbers=("NDHWC", "DHWIO", "NDHWC"), preferred_element_type=jnp.float32)
    activated = (features.astype(jnp.float32) + jax.nn.silu(conv)).astype(jnp.bfloat16)
    latent = jnp.einsum("bfyxc,cl->bfyxl", activated.astype(jnp.float32), latent_weight.astype(jnp.float32)).astype(jnp.bfloat16)
    clips = latent.shape[0]
    frames = latent.shape[1]
    rows = latent.shape[2] // 2
    cols = latent.shape[3] // 2
    patches = latent.reshape(clips, frames, rows, 2, cols, 2, LAT).transpose(0, 1, 2, 4, 3, 5, 6)
    patches = patches.reshape(clips, frames, N_SEQ, rows // N_SEQ, cols, 4 * LAT).transpose(0, 2, 1, 3, 4, 5)
    patches = patches.reshape(clips, N_SEQ, -1, 4 * LAT)
    tokens = jnp.take(patches, order, axis=2).reshape(-1, 4 * LAT)
    embedded = jnp.dot(tokens, embed_weight, preferred_element_type=jnp.float32).astype(jnp.bfloat16)
    grad = jnp.dot(tokens.T, cotangent, preferred_element_type=jnp.float32)
    embed_grad = grad.reshape(4 * LAT, N_MP, -1).transpose(1, 0, 2)
    return embedded, embed_grad
```

```python
import jax
import jax.numpy as jnp
from jax import lax
from jax.experimental import pallas as pl
from jax.experimental.pallas import tpu as pltpu
from jax.sharding import PartitionSpec as P

MESH = pl.DeviceIdType.MESH
BF16, F32 = jnp.bfloat16, jnp.float32
NX, NY, NZH, NZL = 4, 8, 3, 4
NZ = NZH * NZL
N_SEQ, N_MP = 16, 2
GROUP = N_SEQ * N_MP
FRAMES = 32


def div(a, b):
    return lax.div(a, jnp.int32(b))


def rem(a, b):
    return lax.rem(a, jnp.int32(b))


def kernel(
    feat_hbm, w_hbm, wl_hbm, order_hbm, emb_hbm, cot_hbm,
    embedded_ref, grad_ref,
    feat, w, wl, order, emb, cot, halo, shifted, acc, act, wl4, perm_t, perm, cot_t,
    tokbuf, tokin, gsend, xrecv, ysend, yrecv, zsend, zrecv,
    load_sem, halo_send, halo_recv, tok_send, tok_recv,
    x_send, x_recv, y_send, y_recv, z_send, z_recv,
):
    dp, seq, mp = lax.axis_index("dp"), lax.axis_index("seq"), lax.axis_index("mp")
    x, zl = rem(seq, NX), div(seq, NX)
    y, zh = rem(dp, NY), div(dp, NY)
    z = zh * NZL + zl
    me = seq * N_MP + mp
    frame = me + 1
    slab_peer = seq + 2 * mp - 1
    has_peer = jnp.logical_and(slab_peer >= 0, slab_peer < N_SEQ)
    partner = (dp, seq, 1 - mp)

    def x_peer(k):
        tx = rem(x + k, NX)
        return tx, (dp, zl * NX + tx, mp)

    def y_peer(k):
        ty = rem(y + k, NY)
        return ty, (zh * NY + ty, seq, mp)

    def z_peer(k):
        tz = rem(z + k, NZ)
        th, tl = div(tz, NZL), rem(tz, NZL)
        return th * 2 + div(tl, 2), (th * NY + y, tl * NX + x, mp)

    def group_peer(k):
        index = rem(me + k, GROUP)
        return div(index, N_MP), (dp, div(index, N_MP), rem(index, N_MP))

    loads = [
        pltpu.make_async_copy(src, dst, load_sem.at[i])
        for i, (src, dst) in enumerate(
            [(feat_hbm.at[0], feat), (w_hbm, w), (wl_hbm, wl), (order_hbm, order), (cot_hbm, cot), (emb_hbm, emb)]
        )
    ]
    for load in loads:
        load.start()

    barrier = pltpu.get_barrier_semaphore()

    def greet(k, carry):
        pl.semaphore_signal(barrier, inc=1, device_id=group_peer(k)[1], device_id_type=MESH)
        return carry

    lax.fori_loop(1, GROUP, greet, 0)
    for k in range(1, NY):
        pl.semaphore_signal(barrier, inc=1, device_id=y_peer(k)[1], device_id_type=MESH)
    for k in range(1, NZ):
        pl.semaphore_signal(barrier, inc=1, device_id=z_peer(k)[1], device_id_type=MESH)
    loads[0].wait()
    pl.semaphore_wait(barrier, GROUP - 1 + NY - 1 + NZ - 1)

    halo_copy = pltpu.make_async_remote_copy(
        src_ref=feat.at[mp], dst_ref=halo, send_sem=halo_send, recv_sem=halo_recv,
        device_id=(dp, slab_peer, 1 - mp), device_id_type=MESH,
    )

    @pl.when(has_peer)
    def _():
        halo_copy.start()

    def shift(slot, value):
        value = value.astype(F32)
        zero = jnp.zeros((FRAMES, 1, 256), F32)
        shifted[slot, 0, 1:33] = jnp.concatenate([zero, value[:, :15]], axis=1).astype(BF16)
        shifted[slot, 1, 1:33] = value.astype(BF16)
        shifted[slot, 2, 1:33] = jnp.concatenate([value[:, 1:], zero], axis=1).astype(BF16)

    for slot in range(3):
        for dx in range(3):
            shifted[slot, dx, 0] = jnp.zeros((16, 256), BF16)
            shifted[slot, dx, 33] = jnp.zeros((16, 256), BF16)

    def taps(slot, dt):
        total = None
        for dy in range(3):
            for dx in range(3):
                part = jnp.dot(
                    shifted[slot, dx, dy : dy + 32].reshape(512, 256), w[dt, dy, dx],
                    preferred_element_type=F32,
                )
                total = part if total is None else total + part
        return total.reshape(32, 16, 256)

    shift(0, feat[0])
    shift(1, feat[1])
    loads[1].wait()
    acc[0] = taps(0, 1 - mp) + taps(1, 2 - mp)
    acc[1] = jnp.zeros((32, 16, 256), F32)

    loads[2].wait()
    wl4[...] = jnp.zeros((4, 64, 256), BF16)
    for k in range(4):
        wl4[k, 16 * k : 16 * k + 16] = wl[...]
    loads[3].wait()
    hot = jnp.where(lax.broadcasted_iota(jnp.int32, (256, 256), 0) == order[...], 1.0, 0.0).astype(F32)
    perm_t[...] = hot.astype(BF16)
    perm[...] = hot.T.astype(BF16)

    first = frame == 1

    @pl.when(has_peer)
    def _():
        halo_copy.wait_recv()

    @pl.when(jnp.logical_not(has_peer))
    def _():
        halo[...] = jnp.zeros((32, 16, 256), BF16)

    shift(2, halo[...])
    slot3 = jnp.where(first, 0, 2)
    dt3 = jnp.where(first, 2, 2 * mp)
    dst3 = jnp.where(first, 1, 0)
    acc[dst3] += taps(slot3, dt3)

    def to_tokens(slot, source):
        value = source.astype(F32) + jax.nn.silu(acc[slot])
        for c in range(2):
            act[c] = value[:, :, 128 * c : 128 * c + 128]
        total = None
        for dx in range(2):
            half = jnp.concatenate(
                [act[c, :, pl.ds(dx, 8, stride=2), :] for c in range(2)], axis=-1
            ).reshape(16, 2, 8, 256)
            for dy in range(2):
                part = lax.dot_general(
                    half[:, dy].reshape(128, 256).astype(BF16), wl4[2 * dy + dx],
                    (((1,), (1,)), ((), ())), preferred_element_type=F32,
                )
                total = part if total is None else total + part
        tokbuf[slot] = total.reshape(16, 8, 64).astype(BF16)

    def token_copy(slot, to, k):
        band, device = group_peer(k)
        return pltpu.make_async_remote_copy(
            src_ref=tokbuf.at[slot, band], dst_ref=tokin.at[to],
            send_sem=tok_send.at[slot, k], recv_sem=tok_recv.at[to],
            device_id=device, device_id_type=MESH,
        )

    def send_tokens(slot, to):
        def step(k, carry):
            token_copy(slot, to, k).start()
            return carry

        lax.fori_loop(1, GROUP, step, 0)
        tokin[to] = tokbuf[slot, seq]

    @pl.when(mp == 0)
    def _():
        to_tokens(0, feat[1])

    @pl.when(mp == 1)
    def _():
        to_tokens(0, halo[...])

    @pl.when(frame < FRAMES)
    def _():
        send_tokens(0, frame)

    @pl.when(first)
    def _():
        to_tokens(1, feat[0])
        send_tokens(1, 0)

    loads[4].wait()
    for block in range(NY * NZH):
        moved = jnp.dot(perm_t[...], cot[:, 128 * block : 128 * block + 128], preferred_element_type=F32)
        turned = moved.T.reshape(2, 2, NX, 8, 256)
        for one in range(2):
            for tx in range(NX):
                cot_t[one, tx, block % NY, block // NY] = jnp.concatenate(
                    [turned[0, one, tx], turned[1, one, tx]], axis=0
                ).astype(BF16)

    def token_wait(f, carry):
        own = jnp.logical_or(frame == f, jnp.logical_and(first, f == 0))

        @pl.when(jnp.logical_not(own))
        def _():
            pltpu.make_async_remote_copy(
                src_ref=tokbuf.at[0, 0], dst_ref=tokin.at[f],
                send_sem=tok_send.at[0, 0], recv_sem=tok_recv.at[f],
                device_id=partner, device_id_type=MESH,
            ).wait_recv()

        return carry

    lax.fori_loop(0, FRAMES, token_wait, 0)
    tok = tokin[...].astype(F32).reshape(256, 64)
    zero = jnp.zeros((256, 64), F32)
    tok_a = jnp.concatenate([tok, zero], axis=1).astype(BF16)
    tok_b = jnp.concatenate([zero, tok], axis=1).astype(BF16)

    def x_copy(k):
        tx, device = x_peer(k)
        return pltpu.make_async_remote_copy(
            src_ref=gsend.at[tx], dst_ref=xrecv.at[k - 1],
            send_sem=x_send.at[k - 1], recv_sem=x_recv.at[k - 1],
            device_id=device, device_id_type=MESH,
        )

    for k in (2, 1, 3, 0):
        tx = rem(x + k, NX)
        gsend[tx] = (
            jnp.dot(cot_t[0, tx].reshape(384, 256), tok_a, preferred_element_type=F32)
            + jnp.dot(cot_t[1, tx].reshape(384, 256), tok_b, preferred_element_type=F32)
        ).astype(BF16)
        if k:
            x_copy(k).start()

    loads[5].wait()
    ordered = jnp.dot(perm[...], tok.astype(BF16), preferred_element_type=F32).astype(BF16)
    for c in range(0, 3072, 512):
        embedded_ref[:, c : c + 512] = jnp.dot(
            ordered, emb[:, c : c + 512], preferred_element_type=F32
        ).astype(BF16)

    for k in range(1, NX):
        x_copy(k).wait_recv()
    total = gsend[x].astype(F32)
    for k in range(1, NX):
        total += xrecv[k - 1].astype(F32)
    ysend[...] = total.reshape(NY, 48, 128).astype(BF16)

    def y_copy(k):
        ty, device = y_peer(k)
        return pltpu.make_async_remote_copy(
            src_ref=ysend.at[ty], dst_ref=yrecv.at[k - 1],
            send_sem=y_send.at[k - 1], recv_sem=y_recv.at[k - 1],
            device_id=device, device_id_type=MESH,
        )

    for k in (4, 3, 5, 2, 6, 1, 7):
        y_copy(k).start()
    for k in range(1, NY):
        y_copy(k).wait_recv()
    total = ysend[y].astype(F32)
    for k in range(1, NY):
        total += yrecv[k - 1].astype(F32)
    zsend[...] = total.reshape(6, 8, 128).astype(BF16)

    def z_copy(k):
        piece, device = z_peer(k)
        return pltpu.make_async_remote_copy(
            src_ref=zsend.at[piece], dst_ref=zrecv.at[k - 1],
            send_sem=z_send.at[k - 1], recv_sem=z_recv.at[k - 1],
            device_id=device, device_id_type=MESH,
        )

    for k in (6, 5, 7, 4, 8, 3, 9, 2, 10, 1, 11):
        z_copy(k).start()
    for k in range(1, NZ):
        z_copy(k).wait_recv()
    total = zsend[zh * 2 + div(zl, 2)].astype(F32)
    for k in range(1, NZ):
        total += zrecv[k - 1].astype(F32)
    grad_ref[...] = jnp.where(rem(zl, 2) == 0, total[:, :64], total[:, 64:])

    @pl.when(has_peer)
    def _():
        halo_copy.wait_send()

    def drain(slot, to):
        def step(k, carry):
            token_copy(slot, to, k).wait_send()
            return carry

        lax.fori_loop(1, GROUP, step, 0)

    @pl.when(frame < FRAMES)
    def _():
        drain(0, frame)

    @pl.when(first)
    def _():
        drain(1, 0)

    for k in range(1, NX):
        x_copy(k).wait_send()
    for k in range(1, NY):
        y_copy(k).wait_send()
    for k in range(1, NZ):
        z_copy(k).wait_send()


def local(features, conv_weight, latent_weight, order, embed_weight, cotangent):
    dma = pltpu.SemaphoreType.DMA
    embedded, grad = pl.pallas_call(
        kernel,
        name="section",
        out_shape=(
            jax.ShapeDtypeStruct((256, 3072), BF16),
            jax.ShapeDtypeStruct((8, 64), F32),
        ),
        in_specs=[pl.BlockSpec(memory_space=pl.ANY)] * 6,
        out_specs=(pl.BlockSpec(memory_space=pltpu.VMEM),) * 2,
        scratch_shapes=[
            pltpu.VMEM((2, 32, 16, 256), BF16),
            pltpu.VMEM((3, 3, 3, 256, 256), BF16),
            pltpu.VMEM((16, 256), BF16),
            pltpu.VMEM((1, 256), jnp.int32),
            pltpu.VMEM((64, 3072), BF16),
            pltpu.VMEM((256, 3072), BF16),
            pltpu.VMEM((32, 16, 256), BF16),
            pltpu.VMEM((3, 3, 34, 16, 256), BF16),
            pltpu.VMEM((2, 32, 16, 256), F32),
            pltpu.VMEM((2, 32, 16, 128), F32),
            pltpu.VMEM((4, 64, 256), BF16),
            pltpu.VMEM((256, 256), BF16),
            pltpu.VMEM((256, 256), BF16),
            pltpu.VMEM((2, NX, NY, NZH, 16, 256), BF16),
            pltpu.VMEM((2, 16, 8, 64), BF16),
            pltpu.VMEM((32, 8, 64), BF16),
            pltpu.VMEM((NX, 384, 128), BF16),
            pltpu.VMEM((NX - 1, 384, 128), BF16),
            pltpu.VMEM((NY, 48, 128), BF16),
            pltpu.VMEM((NY - 1, 48, 128), BF16),
            pltpu.VMEM((6, 8, 128), BF16),
            pltpu.VMEM((NZ - 1, 8, 128), BF16),
            dma((6,)),
            dma, dma,
            dma((2, GROUP)), dma((FRAMES,)),
            dma((NX - 1,)), dma((NX - 1,)),
            dma((NY - 1,)), dma((NY - 1,)),
            dma((NZ - 1,)), dma((NZ - 1,)),
        ],
        compiler_params=pltpu.CompilerParams(collective_id=0, has_side_effects=True),
    )(features, conv_weight, latent_weight.T, order.reshape(1, 256), embed_weight, cotangent)
    return embedded, grad.T[None]


def solution(mesh):
    placed = (
        P("dp", "seq", None, None, None),
        P(),
        P(),
        P(),
        P(None, "mp"),
        P(("dp", "seq"), "mp"),
    )
    return jax.shard_map(
        local,
        mesh=mesh,
        in_specs=placed,
        out_specs=(P(("dp", "seq"), "mp"), P("mp", None, ("dp", "seq"))),
        check_vma=False,
    )
```

```python
import jax
import jax.numpy as jnp
from jax import lax
from jax.experimental import pallas as pl
from jax.experimental.pallas import tpu as pltpu
from jax.sharding import PartitionSpec as P

MESH = pl.DeviceIdType.MESH
BF16, F32 = jnp.bfloat16, jnp.float32
NX, NY, NZH, NZL = 4, 8, 3, 4
NZ = NZH * NZL
N_SEQ, N_MP = 16, 2
GROUP = N_SEQ * N_MP
FRAMES = 32


def div(a, b):
    return lax.div(a, jnp.int32(b))


def rem(a, b):
    return lax.rem(a, jnp.int32(b))


def kernel(
    feat_hbm, w_hbm, wl_hbm, order_hbm, cot_hbm, emb_hbm,
    embedded_ref, grad_ref,
    feat, w, wl, order, cot, emb, halo, shifted, acc, act, wl4, perm_t, perm, cot_t,
    tokbuf, tokin, gsend, xrecv, ysend, yrecv, zsend, zrecv,
    load_sem, halo_send, halo_recv, tok_send, tok_recv,
    x_send, x_recv, y_send, y_recv, z_send, z_recv,
):
    dp, seq, mp = lax.axis_index("dp"), lax.axis_index("seq"), lax.axis_index("mp")
    x, zl = rem(seq, NX), div(seq, NX)
    y, zh = rem(dp, NY), div(dp, NY)
    z = zh * NZL + zl
    me = seq * N_MP + mp
    frame = me + 1
    slab_peer = seq + 2 * mp - 1
    has_peer = jnp.logical_and(slab_peer >= 0, slab_peer < N_SEQ)
    partner = (dp, seq, 1 - mp)

    def x_peer(k):
        tx = rem(x + k, NX)
        return tx, (dp, zl * NX + tx, mp)

    def y_peer(k):
        ty = rem(y + k, NY)
        return ty, (zh * NY + ty, seq, mp)

    def z_device(tz):
        return div(tz, NZL) * NY + y, rem(tz, NZL) * NX + x, mp

    def group_peer(k):
        index = rem(me + k, GROUP)
        return div(index, N_MP), (dp, div(index, N_MP), rem(index, N_MP))

    loads = [
        pltpu.make_async_copy(src, dst, load_sem.at[i])
        for i, (src, dst) in enumerate(
            [(feat_hbm.at[0], feat), (w_hbm, w), (wl_hbm, wl), (order_hbm, order), (cot_hbm, cot), (emb_hbm, emb)]
        )
    ]
    for load in loads:
        load.start()

    barrier = pltpu.get_barrier_semaphore()

    def greet(k, carry):
        pl.semaphore_signal(barrier, inc=1, device_id=group_peer(k)[1], device_id_type=MESH)
        return carry

    lax.fori_loop(1, GROUP, greet, 0)
    for k in range(1, NY):
        pl.semaphore_signal(barrier, inc=1, device_id=y_peer(k)[1], device_id_type=MESH)
    for k in range(1, NZ):
        pl.semaphore_signal(barrier, inc=1, device_id=z_device(rem(z + k, NZ)), device_id_type=MESH)
    loads[0].wait()
    pl.semaphore_wait(barrier, GROUP - 1 + NY - 1 + NZ - 1)

    halo_copy = pltpu.make_async_remote_copy(
        src_ref=feat.at[mp], dst_ref=halo, send_sem=halo_send, recv_sem=halo_recv,
        device_id=(dp, slab_peer, 1 - mp), device_id_type=MESH,
    )

    @pl.when(has_peer)
    def _():
        halo_copy.start()

    def shift(slot, value):
        value = value.astype(F32)
        zero = jnp.zeros((FRAMES, 1, 256), F32)
        shifted[slot, 0, 1:33] = jnp.concatenate([zero, value[:, :15]], axis=1).astype(BF16)
        shifted[slot, 1, 1:33] = value.astype(BF16)
        shifted[slot, 2, 1:33] = jnp.concatenate([value[:, 1:], zero], axis=1).astype(BF16)

    for slot in range(3):
        for dx in range(3):
            shifted[slot, dx, 0] = jnp.zeros((16, 256), BF16)
            shifted[slot, dx, 33] = jnp.zeros((16, 256), BF16)

    def taps(slot, dt):
        total = None
        for dy in range(3):
            for dx in range(3):
                part = jnp.dot(
                    shifted[slot, dx, dy : dy + 32].reshape(512, 256), w[dt, dy, dx],
                    preferred_element_type=F32,
                )
                total = part if total is None else total + part
        return total.reshape(32, 16, 256)

    shift(0, feat[0])
    shift(1, feat[1])
    loads[1].wait()
    acc[0] = taps(0, 1 - mp) + taps(1, 2 - mp)
    acc[1] = jnp.zeros((32, 16, 256), F32)

    loads[2].wait()
    wl4[...] = jnp.zeros((4, 64, 256), BF16)
    for k in range(4):
        wl4[k, 16 * k : 16 * k + 16] = wl[...]
    loads[3].wait()
    hot = jnp.where(lax.broadcasted_iota(jnp.int32, (256, 256), 0) == order[...], 1.0, 0.0).astype(F32)
    perm_t[...] = hot.astype(BF16)
    perm[...] = hot.T.astype(BF16)

    first = frame == 1

    @pl.when(has_peer)
    def _():
        halo_copy.wait_recv()

    @pl.when(jnp.logical_not(has_peer))
    def _():
        halo[...] = jnp.zeros((32, 16, 256), BF16)

    shift(2, halo[...])
    slot3 = jnp.where(first, 0, 2)
    dt3 = jnp.where(first, 2, 2 * mp)
    dst3 = jnp.where(first, 1, 0)
    acc[dst3] += taps(slot3, dt3)

    def to_tokens(slot, source):
        value = source.astype(F32) + jax.nn.silu(acc[slot])
        for c in range(2):
            act[c] = value[:, :, 128 * c : 128 * c + 128]
        total = None
        for dx in range(2):
            half = jnp.concatenate(
                [act[c, :, pl.ds(dx, 8, stride=2), :] for c in range(2)], axis=-1
            ).reshape(16, 2, 8, 256)
            for dy in range(2):
                part = lax.dot_general(
                    half[:, dy].reshape(128, 256).astype(BF16), wl4[2 * dy + dx],
                    (((1,), (1,)), ((), ())), preferred_element_type=F32,
                )
                total = part if total is None else total + part
        tokbuf[slot] = total.reshape(16, 8, 64).astype(BF16)

    def token_copy(slot, to, k):
        band, device = group_peer(k)
        return pltpu.make_async_remote_copy(
            src_ref=tokbuf.at[slot, band], dst_ref=tokin.at[to],
            send_sem=tok_send.at[slot, k], recv_sem=tok_recv.at[to],
            device_id=device, device_id_type=MESH,
        )

    def send_tokens(slot, to):
        def step(k, carry):
            token_copy(slot, to, k).start()
            return carry

        lax.fori_loop(1, GROUP, step, 0)
        tokin[to] = tokbuf[slot, seq]

    @pl.when(mp == 0)
    def _():
        to_tokens(0, feat[1])

    @pl.when(mp == 1)
    def _():
        to_tokens(0, halo[...])

    @pl.when(frame < FRAMES)
    def _():
        send_tokens(0, frame)

    @pl.when(first)
    def _():
        to_tokens(1, feat[0])
        send_tokens(1, 0)

    loads[4].wait()
    for block in range(NZH * NY // 2):
        zh_of, y_of = block // (NY // 2), 2 * (block % (NY // 2))
        moved = jnp.dot(perm_t[...], cot[:, 256 * block : 256 * block + 256], preferred_element_type=F32)
        turned = moved.T.reshape(2, 2, 2, NX, 8, 256)
        for pair in range(2):
            for one in range(2):
                for tx in range(NX):
                    cot_t[2 * zh_of + pair, one, tx, 8 * y_of : 8 * y_of + 16] = jnp.concatenate(
                        [turned[0, pair, one, tx], turned[1, pair, one, tx]], axis=0
                    ).astype(BF16)

    def token_wait(f, carry):
        own = jnp.logical_or(frame == f, jnp.logical_and(first, f == 0))

        @pl.when(jnp.logical_not(own))
        def _():
            pltpu.make_async_remote_copy(
                src_ref=tokbuf.at[0, 0], dst_ref=tokin.at[f],
                send_sem=tok_send.at[0, 0], recv_sem=tok_recv.at[f],
                device_id=partner, device_id_type=MESH,
            ).wait_recv()

        return carry

    lax.fori_loop(0, FRAMES, token_wait, 0)
    tok = tokin[...].astype(F32).reshape(256, 64)
    zero = jnp.zeros((256, 64), F32)
    tok_a = jnp.concatenate([tok, zero], axis=1).astype(BF16)
    tok_b = jnp.concatenate([zero, tok], axis=1).astype(BF16)

    far_first = (3, 2, 4, 1, 5, 0)
    pair = div(z, 2)

    def x_copy(o, k):
        tx, device = x_peer(k)
        return pltpu.make_async_remote_copy(
            src_ref=gsend.at[o, tx], dst_ref=xrecv.at[o, k - 1],
            send_sem=x_send.at[o, k - 1], recv_sem=x_recv.at[o, k - 1],
            device_id=device, device_id_type=MESH,
        )

    for o, off in enumerate(far_first):
        c = rem(pair + off, NZ // 2)
        gsend[o] = (
            jnp.dot(cot_t[c, 0].reshape(256, 256), tok_a, preferred_element_type=F32)
            + jnp.dot(cot_t[c, 1].reshape(256, 256), tok_b, preferred_element_type=F32)
        ).astype(BF16).reshape(NX, 64, 128)
        for k in (2, 1, 3):
            x_copy(o, k).start()

    loads[5].wait()
    ordered = jnp.dot(perm[...], tok.astype(BF16), preferred_element_type=F32).astype(BF16)
    for i in range(0, 3072, 512):
        embedded_ref[:, i : i + 512] = jnp.dot(
            ordered, emb[:, i : i + 512], preferred_element_type=F32
        ).astype(BF16)

    def y_copy(o, k):
        ty, device = y_peer(k)
        return pltpu.make_async_remote_copy(
            src_ref=ysend.at[o, ty], dst_ref=yrecv.at[o, k - 1],
            send_sem=y_send.at[o, k - 1], recv_sem=y_recv.at[o, k - 1],
            device_id=device, device_id_type=MESH,
        )

    for o in range(6):
        total = gsend[o, x].astype(F32)
        for k in range(1, NX):
            x_copy(o, k).wait_recv()
            total += xrecv[o, k - 1].astype(F32)
        ysend[o] = total.reshape(NY, 8, 128).astype(BF16)
        for k in (4, 3, 5, 2, 6, 1, 7):
            y_copy(o, k).start()

    def z_copy(o, tz, k):
        return pltpu.make_async_remote_copy(
            src_ref=zsend.at[o], dst_ref=zrecv.at[k - 1],
            send_sem=z_send.at[k - 1], recv_sem=z_recv.at[k - 1],
            device_id=z_device(tz), device_id_type=MESH,
        )

    def z_targets(o):
        c = rem(pair + far_first[o], NZ // 2)
        both = [2 * c, 2 * c + 1] if far_first[o] else [z + 1 - 2 * rem(z, 2)]
        return [(tz, rem(tz - z + NZ, NZ)) for tz in both]

    for o in range(6):
        total = ysend[o, y].astype(F32)
        for k in range(1, NY):
            y_copy(o, k).wait_recv()
            total += yrecv[o, k - 1].astype(F32)
        zsend[o] = total.astype(BF16)
        for tz, k in z_targets(o):
            z_copy(o, tz, k).start()
    for k in range(1, NZ):
        z_copy(0, rem(z + k, NZ), k).wait_recv()
        total += zrecv[k - 1].astype(F32)
    grad_ref[...] = jnp.where(rem(z, 2) == 0, total[:, :64], total[:, 64:])

    @pl.when(has_peer)
    def _():
        halo_copy.wait_send()

    def drain(slot, to):
        def step(k, carry):
            token_copy(slot, to, k).wait_send()
            return carry

        lax.fori_loop(1, GROUP, step, 0)

    @pl.when(frame < FRAMES)
    def _():
        drain(0, frame)

    @pl.when(first)
    def _():
        drain(1, 0)

    for o in range(6):
        for k in range(1, NX):
            x_copy(o, k).wait_send()
        for k in range(1, NY):
            y_copy(o, k).wait_send()
    for k in range(1, NZ):
        z_copy(0, rem(z + k, NZ), k).wait_send()


def finish(embedded_ref, partial_ref, embedded_hbm, grad_hbm, sem):
    copies = [
        pltpu.make_async_copy(embedded_ref, embedded_hbm, sem.at[0]),
        pltpu.make_async_copy(partial_ref, grad_hbm, sem.at[1]),
    ]
    for copy in copies:
        copy.start()
    for copy in copies:
        copy.wait()


def local(features, conv_weight, latent_weight, order, embed_weight, cotangent):
    dma = pltpu.SemaphoreType.DMA
    vmem = pl.BlockSpec(memory_space=pltpu.VMEM)
    embedded, partial = pl.pallas_call(
        kernel,
        name="section",
        out_shape=(
            jax.ShapeDtypeStruct((256, 3072), BF16),
            jax.ShapeDtypeStruct((8, 64), F32),
        ),
        in_specs=[pl.BlockSpec(memory_space=pltpu.HBM)] * 6,
        out_specs=(vmem, vmem),
        scratch_shapes=[
            pltpu.VMEM((2, 32, 16, 256), BF16),
            pltpu.VMEM((3, 3, 3, 256, 256), BF16),
            pltpu.VMEM((16, 256), BF16),
            pltpu.VMEM((1, 256), jnp.int32),
            pltpu.VMEM((256, 3072), BF16),
            pltpu.VMEM((64, 3072), BF16),
            pltpu.VMEM((32, 16, 256), BF16),
            pltpu.VMEM((3, 3, 34, 16, 256), BF16),
            pltpu.VMEM((2, 32, 16, 256), F32),
            pltpu.VMEM((2, 32, 16, 128), F32),
            pltpu.VMEM((4, 64, 256), BF16),
            pltpu.VMEM((256, 256), BF16),
            pltpu.VMEM((256, 256), BF16),
            pltpu.VMEM((6, 2, NX, 64, 256), BF16),
            pltpu.VMEM((2, 16, 8, 64), BF16),
            pltpu.VMEM((32, 8, 64), BF16),
            pltpu.VMEM((6, NX, 64, 128), BF16),
            pltpu.VMEM((6, NX - 1, 64, 128), BF16),
            pltpu.VMEM((6, NY, 8, 128), BF16),
            pltpu.VMEM((6, NY - 1, 8, 128), BF16),
            pltpu.VMEM((6, 8, 128), BF16),
            pltpu.VMEM((NZ - 1, 8, 128), BF16),
            dma((6,)),
            dma, dma,
            dma((2, GROUP)), dma((FRAMES,)),
            dma((6, NX - 1)), dma((6, NX - 1)),
            dma((6, NY - 1)), dma((6, NY - 1)),
            dma((NZ - 1,)), dma((NZ - 1,)),
        ],
        compiler_params=pltpu.CompilerParams(
            collective_id=0, has_side_effects=True, vmem_limit_bytes=32 * 1024 * 1024
        ),
    )(
        *(
            pltpu.with_memory_space_constraint(value, pltpu.HBM)
            for value in (features, conv_weight, latent_weight.T, order.reshape(1, 256), cotangent, embed_weight)
        )
    )
    embedded, grad = pl.pallas_call(
        finish,
        name="finish",
        out_shape=(
            jax.ShapeDtypeStruct((256, 3072), BF16),
            jax.ShapeDtypeStruct((8, 64), F32),
        ),
        in_specs=[vmem] * 2,
        out_specs=(pl.BlockSpec(memory_space=pltpu.HBM),) * 2,
        scratch_shapes=[dma((2,))],
        compiler_params=pltpu.CompilerParams(vmem_limit_bytes=16 * 1024 * 1024),
    )(embedded, partial)
    return embedded, grad.T[None]


def solution(mesh):
    placed = (
        P("dp", "seq", None, None, None),
        P(),
        P(),
        P(),
        P(None, "mp"),
        P(("dp", "seq"), "mp"),
    )
    return jax.shard_map(
        local,
        mesh=mesh,
        in_specs=placed,
        out_specs=(P(("dp", "seq"), "mp"), P("mp", None, ("dp", "seq"))),
        check_vma=False,
    )
```

```python
import jax
import jax.numpy as jnp
from jax import lax
from jax.experimental import pallas as pl
from jax.experimental.pallas import tpu as pltpu
from jax.sharding import PartitionSpec as P

MESH = pl.DeviceIdType.MESH
BF16, F32 = jnp.bfloat16, jnp.float32
NX, NY, NZH, NZL = 4, 8, 3, 4
NZ = NZH * NZL
N_SEQ, N_MP = 16, 2
GROUP = N_SEQ * N_MP
FRAMES = 32
DEPTH = 6


def div(a, b):
    return lax.div(a, jnp.int32(b))


def rem(a, b):
    return lax.rem(a, jnp.int32(b))


def kernel(
    feat_hbm, w_hbm, wl_hbm, order_hbm, cot_hbm, emb_hbm,
    embedded_ref, grad_ref,
    feat, w, wl, order, cot, emb, halo, shifted, acc, act, wl4, perm_t, perm, cot_t,
    tokbuf, tokin, gsend, xrecv, ysend, yzrecv,
    load_sem, halo_send, halo_recv, tok_send, tok_recv,
    x_send, x_recv, yz_send, yz_recv, met,
):
    dp, seq, mp = lax.axis_index("dp"), lax.axis_index("seq"), lax.axis_index("mp")
    x, zl = rem(seq, NX), div(seq, NX)
    y, zh = rem(dp, NY), div(dp, NY)
    z = zh * NZL + zl
    me = seq * N_MP + mp
    frame = me + 1
    slab_peer = seq + 2 * mp - 1
    has_peer = jnp.logical_and(slab_peer >= 0, slab_peer < N_SEQ)
    partner = (dp, seq, 1 - mp)

    def x_peer(k):
        tx = rem(x + k, NX)
        return tx, (dp, zl * NX + tx, mp)

    def member(index):
        return div(index, N_MP), (dp, div(index, N_MP), rem(index, N_MP))

    loads = [
        pltpu.make_async_copy(src, dst, load_sem.at[i])
        for i, (src, dst) in enumerate(
            [(feat_hbm.at[0], feat), (w_hbm, w), (wl_hbm, wl), (order_hbm, order), (cot_hbm, cot), (emb_hbm, emb)]
        )
    ]
    for load in loads:
        load.start()

    def line_device(dy, dz):
        ty, tz = rem(y + dy + NY, NY), rem(z + dz + NZ, NZ)
        return div(tz, NZL) * NY + ty, rem(tz, NZL) * NX + x, mp

    def signal(sem, device):
        pl.semaphore_signal(sem, inc=1, device_id=device, device_id_type=MESH)

    def tell(sem, offsets):
        for dy, dz in offsets:
            signal(sem, line_device(dy, dz))

    near = [(0, 1), (0, -1), (1, 0), (-1, 0)]
    barrier = pltpu.get_barrier_semaphore()
    slab_device = (dp, slab_peer, 1 - mp)

    @pl.when(has_peer)
    def _():
        signal(barrier, slab_device)

    for k in range(1, NX):
        signal(barrier, (dp, zl * NX + rem(x + k, NX), mp))
    for k in range(NX):
        signal(barrier, (dp, zl * NX + rem(x + k, NX), 1 - mp))
    tell(barrier, near)
    loads[0].wait()
    pl.semaphore_wait(barrier, jnp.where(has_peer, 12, 11))

    parts = (slice(0, 17), slice(17, 32))
    halo_copies = [
        pltpu.make_async_remote_copy(
            src_ref=feat.at[mp, rows], dst_ref=halo.at[rows], send_sem=halo_send.at[h], recv_sem=halo_recv.at[h],
            device_id=slab_device, device_id_type=MESH,
        )
        for h, rows in enumerate(parts)
    ]

    @pl.when(has_peer)
    def _():
        for copy in halo_copies:
            copy.start()

    tell(met.at[0], near)

    def shift(slot, source, rows):
        value = source[rows].astype(F32)
        zero = jnp.zeros((rows.stop - rows.start, 1, 256), F32)
        put = slice(1 + rows.start, 1 + rows.stop)
        shifted[slot, 0, put] = jnp.concatenate([zero, value[:, :15]], axis=1).astype(BF16)
        shifted[slot, 1, put] = value.astype(BF16)
        shifted[slot, 2, put] = jnp.concatenate([value[:, 1:], zero], axis=1).astype(BF16)

    for slot in range(3):
        for dx in range(3):
            shifted[slot, dx, 0] = jnp.zeros((16, 256), BF16)
            shifted[slot, dx, 33] = jnp.zeros((16, 256), BF16)

    def taps(slot, dt, first_row, rows):
        total = None
        for dy in range(3):
            for dx in range(3):
                part = jnp.dot(
                    shifted[slot, dx, first_row + dy : first_row + dy + rows].reshape(16 * rows, 256),
                    w[dt, dy, dx], preferred_element_type=F32,
                )
                total = part if total is None else total + part
        return total.reshape(rows, 16, 256)

    shift(0, feat.at[0], slice(0, 32))
    shift(1, feat.at[1], slice(0, 32))
    loads[1].wait()
    acc[0] = taps(0, 1 - mp, 0, 32) + taps(1, 2 - mp, 0, 32)
    acc[1] = jnp.zeros((32, 16, 256), F32)

    pl.semaphore_wait(met.at[0], 4)
    tell(met.at[1], [(0, 2), (0, -2), (2, 0), (-2, 0)])

    loads[2].wait()
    wl4[...] = jnp.zeros((4, 128, 256), BF16)
    for k in range(4):
        wl4[k, 16 * k : 16 * k + 16] = wl[...]
    loads[3].wait()
    hot = jnp.where(lax.broadcasted_iota(jnp.int32, (256, 256), 0) == order[...], 1.0, 0.0).astype(F32)
    perm_t[...] = hot.astype(BF16)
    perm[...] = hot.T.astype(BF16)

    first = frame == 1
    slot3 = jnp.where(first, 0, 2)
    dt3 = jnp.where(first, 2, 2 * mp)
    dst3 = jnp.where(first, 1, 0)

    def to_tokens(slot, source, h):
        half = slice(16 * h, 16 * h + 16)
        value = source[half].astype(F32) + jax.nn.silu(acc[slot, half])
        for c in range(2):
            act[c] = value[:, :, 128 * c : 128 * c + 128]
        total = None
        for dx in range(2):
            columns = jnp.concatenate(
                [act[c, :, pl.ds(dx, 8, stride=2), :] for c in range(2)], axis=-1
            ).reshape(8, 2, 8, 256)
            for dy in range(2):
                part = lax.dot_general(
                    columns[:, dy].reshape(64, 256).astype(BF16), wl4[2 * dy + dx],
                    (((1,), (1,)), ((), ())), preferred_element_type=F32,
                )
                total = part if total is None else total + part
        tokbuf[slot, 8 * h : 8 * h + 8] = total.reshape(8, 8, 128).astype(BF16)

    def token_copy(slot, to, index):
        band, device = member(index)
        return pltpu.make_async_remote_copy(
            src_ref=tokbuf.at[slot, band], dst_ref=tokin.at[to],
            send_sem=tok_send.at[slot, index], recv_sem=tok_recv.at[to],
            device_id=device, device_id_type=MESH,
        )

    def send_tokens(slot, to, h):
        def step(k, carry):
            index = 16 * h + rem(me + k, 16)

            @pl.when(index != me)
            def _():
                token_copy(slot, to, index).start()

            return carry

        lax.fori_loop(0, 16, step, 0)

    pl.semaphore_wait(met.at[1], 4)
    tell(met.at[2], [(0, 4), (0, -4)])
    for h in range(2):
        @pl.when(has_peer)
        def _():
            halo_copies[h].wait_recv()

        @pl.when(jnp.logical_not(has_peer))
        def _():
            halo[parts[h]] = jnp.zeros((parts[h].stop - parts[h].start, 16, 256), BF16)

        shift(2, halo, parts[h])
        acc[dst3, 16 * h : 16 * h + 16] += taps(slot3, dt3, 16 * h, 16)

        @pl.when(mp == 0)
        def _():
            to_tokens(0, feat.at[1], h)

        @pl.when(mp == 1)
        def _():
            to_tokens(0, halo, h)

        @pl.when(frame < FRAMES)
        def _():
            send_tokens(0, frame, h)

        @pl.when(first)
        def _():
            to_tokens(1, feat.at[0], h)
            send_tokens(1, 0, h)

    @pl.when(frame < FRAMES)
    def _():
        tokin[frame] = tokbuf[0, seq]

    @pl.when(first)
    def _():
        tokin[0] = tokbuf[1, seq]

    pl.semaphore_wait(met.at[2], 2)
    tell(met.at[3], [(k, 0) for k in range(1, NY)])

    loads[4].wait()
    for block in range(NZH * NY // 2):
        zh_of, y_of = block // (NY // 2), 2 * (block % (NY // 2))
        moved = jnp.dot(perm_t[...], cot[:, 256 * block : 256 * block + 256], preferred_element_type=F32)
        turned = moved.T.reshape(2, 2, 2, NX, 8, 256)
        for pair in range(2):
            for one in range(2):
                for tx in range(NX):
                    cot_t[2 * zh_of + pair, one, tx, 8 * y_of : 8 * y_of + 16] = jnp.concatenate(
                        [turned[0, pair, one, tx], turned[1, pair, one, tx]], axis=0
                    ).astype(BF16)

    def token_wait(f, carry):
        own = jnp.logical_or(frame == f, jnp.logical_and(first, f == 0))

        @pl.when(jnp.logical_not(own))
        def _():
            pltpu.make_async_remote_copy(
                src_ref=tokbuf.at[0, 0], dst_ref=tokin.at[f],
                send_sem=tok_send.at[0, 0], recv_sem=tok_recv.at[f],
                device_id=partner, device_id_type=MESH,
            ).wait_recv()

        return carry

    lax.fori_loop(0, FRAMES, token_wait, 0)
    tok = tokin[...].astype(F32).reshape(256, 128)
    tok_a = tok.astype(BF16)
    tok_b = jnp.concatenate([tok[:, 64:], tok[:, :64]], axis=1).astype(BF16)

    far_first = (3, 2, 4, 1, 5, 0)
    pair = div(z, 2)

    def x_copy(o, k):
        tx, device = x_peer(k)
        return pltpu.make_async_remote_copy(
            src_ref=gsend.at[o, tx], dst_ref=xrecv.at[o, k - 1],
            send_sem=x_send.at[o, k - 1], recv_sem=x_recv.at[o, k - 1],
            device_id=device, device_id_type=MESH,
        )

    def send_x(o):
        c = rem(pair + far_first[o], NZ // 2)
        gsend[o] = (
            jnp.dot(cot_t[c, 0].reshape(256, 256), tok_a, preferred_element_type=F32)
            + jnp.dot(cot_t[c, 1].reshape(256, 256), tok_b, preferred_element_type=F32)
        ).astype(BF16).reshape(NX, 64, 128)
        for k in (2, 1, 3):
            x_copy(o, k).start()

    for o in range(DEPTH):
        send_x(o)

    loads[5].wait()
    ordered = jnp.dot(perm[...], tok_a, preferred_element_type=F32).astype(BF16)[:, :64]
    for i in range(0, 3072, 512):
        embedded_ref[:, i : i + 512] = jnp.dot(
            ordered, emb[:, i : i + 512], preferred_element_type=F32
        ).astype(BF16)

    def plane_copy(o, one, ky):
        tz = 2 * rem(pair + far_first[o], NZ // 2) + one
        slot = rem(tz - z + NZ, NZ) * NY + ky
        ty = rem(y + ky, NY)
        return slot, pltpu.make_async_remote_copy(
            src_ref=ysend.at[o, ty], dst_ref=yzrecv.at[slot],
            send_sem=yz_send.at[o, one, ky], recv_sem=yz_recv.at[slot],
            device_id=(div(tz, NZL) * NY + ty, rem(tz, NZL) * NX + x, mp), device_id_type=MESH,
        )

    def each_plane_copy(o, act_on):
        for ky in (4, 3, 5, 2, 6, 1, 7, 0):
            for one in range(2):
                slot, copy = plane_copy(o, one, ky)
                if far_first[o] or ky:
                    act_on(copy)
                else:
                    @pl.when(slot != 0)
                    def _():
                        act_on(copy)

    pl.semaphore_wait(met.at[3], NY - 1)
    for o in range(6):
        total = gsend[o, x].astype(F32)
        for k in range(1, NX):
            x_copy(o, k).wait_recv()
            total += xrecv[o, k - 1].astype(F32)
        ysend[o] = total.reshape(NY, 8, 128).astype(BF16)
        each_plane_copy(o, lambda copy: copy.start())

    total = ysend[5, y].astype(F32)
    for kz in (0, 1, 11, 2, 10, 3, 9, 4, 8, 5, 7, 6):
        for ky in (0, 1, 7, 2, 6, 3, 5, 4):
            slot = kz * NY + ky
            if slot:
                pltpu.make_async_remote_copy(
                    src_ref=ysend.at[0, 0], dst_ref=yzrecv.at[slot],
                    send_sem=yz_send.at[0, 0, 0], recv_sem=yz_recv.at[slot],
                    device_id=partner, device_id_type=MESH,
                ).wait_recv()
                total += yzrecv[slot].astype(F32)
    grad_ref[...] = jnp.where(rem(z, 2) == 0, total[:, :64], total[:, 64:])

    @pl.when(has_peer)
    def _():
        for copy in halo_copies:
            copy.wait_send()

    def drain(slot, to):
        def step(index, carry):
            @pl.when(index != me)
            def _():
                token_copy(slot, to, index).wait_send()

            return carry

        lax.fori_loop(0, GROUP, step, 0)

    @pl.when(frame < FRAMES)
    def _():
        drain(0, frame)

    @pl.when(first)
    def _():
        drain(1, 0)

    for o in range(6):
        for k in range(1, NX):
            x_copy(o, k).wait_send()
        each_plane_copy(o, lambda copy: copy.wait_send())


def finish(embedded_ref, partial_ref, embedded_hbm, grad_hbm, sem):
    copies = [
        pltpu.make_async_copy(embedded_ref, embedded_hbm, sem.at[0]),
        pltpu.make_async_copy(partial_ref, grad_hbm, sem.at[1]),
    ]
    for copy in copies:
        copy.start()
    for copy in copies:
        copy.wait()


def local(features, conv_weight, latent_weight, order, embed_weight, cotangent):
    dma = pltpu.SemaphoreType.DMA
    vmem = pl.BlockSpec(memory_space=pltpu.VMEM)
    embedded, partial = pl.pallas_call(
        kernel,
        name="section",
        out_shape=(
            jax.ShapeDtypeStruct((256, 3072), BF16),
            jax.ShapeDtypeStruct((8, 64), F32),
        ),
        in_specs=[pl.BlockSpec(memory_space=pltpu.HBM)] * 6,
        out_specs=(vmem, vmem),
        scratch_shapes=[
            pltpu.VMEM((2, 32, 16, 256), BF16),
            pltpu.VMEM((3, 3, 3, 256, 256), BF16),
            pltpu.VMEM((16, 256), BF16),
            pltpu.VMEM((1, 256), jnp.int32),
            pltpu.VMEM((256, 3072), BF16),
            pltpu.VMEM((64, 3072), BF16),
            pltpu.VMEM((32, 16, 256), BF16),
            pltpu.VMEM((3, 3, 34, 16, 256), BF16),
            pltpu.VMEM((2, 32, 16, 256), F32),
            pltpu.VMEM((2, 16, 16, 128), F32),
            pltpu.VMEM((4, 128, 256), BF16),
            pltpu.VMEM((256, 256), BF16),
            pltpu.VMEM((256, 256), BF16),
            pltpu.VMEM((6, 2, NX, 64, 256), BF16),
            pltpu.VMEM((2, 16, 8, 128), BF16),
            pltpu.VMEM((32, 8, 128), BF16),
            pltpu.VMEM((6, NX, 64, 128), BF16),
            pltpu.VMEM((6, NX - 1, 64, 128), BF16),
            pltpu.VMEM((6, NY, 8, 128), BF16),
            pltpu.VMEM((NZ * NY, 8, 128), BF16),
            dma((6,)),
            dma((2,)), dma((2,)),
            dma((2, GROUP)), dma((FRAMES,)),
            dma((6, NX - 1)), dma((6, NX - 1)),
            dma((6, 2, NY)), dma((NZ * NY,)),
            pltpu.SemaphoreType.REGULAR((4,)),
        ],
        compiler_params=pltpu.CompilerParams(
            collective_id=0, has_side_effects=True, vmem_limit_bytes=32 * 1024 * 1024
        ),
    )(
        *(
            pltpu.with_memory_space_constraint(value, pltpu.HBM)
            for value in (features, conv_weight, latent_weight.T, order.reshape(1, 256), cotangent, embed_weight)
        )
    )
    embedded, grad = pl.pallas_call(
        finish,
        name="finish",
        out_shape=(
            jax.ShapeDtypeStruct((256, 3072), BF16),
            jax.ShapeDtypeStruct((8, 64), F32),
        ),
        in_specs=[vmem] * 2,
        out_specs=(pl.BlockSpec(memory_space=pltpu.HBM),) * 2,
        scratch_shapes=[dma((2,))],
        compiler_params=pltpu.CompilerParams(vmem_limit_bytes=16 * 1024 * 1024),
    )(embedded, partial)
    return embedded, grad.T[None]


def solution(mesh):
    placed = (
        P("dp", "seq", None, None, None),
        P(),
        P(),
        P(),
        P(None, "mp"),
        P(("dp", "seq"), "mp"),
    )
    return jax.shard_map(
        local,
        mesh=mesh,
        in_specs=placed,
        out_specs=(P(("dp", "seq"), "mp"), P("mp", None, ("dp", "seq"))),
        check_vma=False,
    )
```

```python
import jax
import jax.numpy as jnp
from jax import lax
from jax.experimental import pallas as pl
from jax.experimental.pallas import tpu as pltpu
from jax.sharding import PartitionSpec as P

MESH = pl.DeviceIdType.MESH
BF16, F32 = jnp.bfloat16, jnp.float32
NX, NY, NZH, NZL = 4, 8, 3, 4
NZ = NZH * NZL
N_SEQ, N_MP = 16, 2
GROUP = N_SEQ * N_MP
FRAMES = 32
DEPTH = 6


def div(a, b):
    return lax.div(a, jnp.int32(b))


def rem(a, b):
    return lax.rem(a, jnp.int32(b))


def kernel(
    feat_hbm, w_hbm, wl_hbm, order_hbm, cot_hbm, emb_hbm,
    embedded_ref, grad_ref,
    feat, w, wl, order, cot, emb, halo, shifted, acc, act, wl4, perm_t, perm, cot_t,
    tokbuf, tokin, gsend, xrecv, ysend, yzrecv,
    load_sem, halo_send, halo_recv, tok_send, tok_recv,
    x_send, x_recv, yz_send, yz_recv, met,
):
    dp, seq, mp = lax.axis_index("dp"), lax.axis_index("seq"), lax.axis_index("mp")
    x, zl = rem(seq, NX), div(seq, NX)
    y, zh = rem(dp, NY), div(dp, NY)
    z = zh * NZL + zl
    me = seq * N_MP + mp
    frame = me + 1
    slab_peer = seq + 2 * mp - 1
    has_peer = jnp.logical_and(slab_peer >= 0, slab_peer < N_SEQ)
    partner = (dp, seq, 1 - mp)

    def x_peer(k):
        tx = rem(x + k, NX)
        return tx, (dp, zl * NX + tx, mp)

    def member(index):
        return div(index, N_MP), (dp, div(index, N_MP), rem(index, N_MP))

    frame_loads = [
        pltpu.make_async_copy(feat_hbm.at[0, i], feat.at[i], load_sem.at[6 + j])
        for j, i in enumerate((mp, 1 - mp))
    ]
    loads = [
        pltpu.make_async_copy(src, dst, load_sem.at[i])
        for i, (src, dst) in enumerate(
            [(w_hbm, w), (wl_hbm, wl), (order_hbm, order), (cot_hbm, cot), (emb_hbm, emb)], 1
        )
    ]
    loads.insert(0, frame_loads[0])
    for load in frame_loads:
        load.start()

    def line_device(dy, dz):
        ty, tz = rem(y + dy + NY, NY), rem(z + dz + NZ, NZ)
        return div(tz, NZL) * NY + ty, rem(tz, NZL) * NX + x, mp

    def signal(sem, device):
        pl.semaphore_signal(sem, inc=1, device_id=device, device_id_type=MESH)

    def tell(sem, offsets):
        for dy, dz in offsets:
            signal(sem, line_device(dy, dz))

    near = [(0, 1), (0, -1), (1, 0), (-1, 0)]
    barrier = pltpu.get_barrier_semaphore()
    slab_device = (dp, slab_peer, 1 - mp)

    @pl.when(has_peer)
    def _():
        signal(barrier, slab_device)

    for k in range(1, NX):
        signal(barrier, (dp, zl * NX + rem(x + k, NX), mp))
    for k in range(NX):
        signal(barrier, (dp, zl * NX + rem(x + k, NX), 1 - mp))
    tell(barrier, near)
    for load in loads[1:4]:
        load.start()
    loads[0].wait()
    pl.semaphore_wait(barrier, jnp.where(has_peer, 12, 11))

    parts = (slice(0, 9), slice(9, 17), slice(17, 25), slice(25, 32))
    halo_copies = [
        pltpu.make_async_remote_copy(
            src_ref=feat.at[mp, rows], dst_ref=halo.at[rows], send_sem=halo_send.at[h], recv_sem=halo_recv.at[h],
            device_id=slab_device, device_id_type=MESH,
        )
        for h, rows in enumerate(parts)
    ]

    @pl.when(has_peer)
    def _():
        for copy in halo_copies:
            copy.start()

    loads[4].start()
    loads[5].start()

    tell(met.at[0], near)

    def shift(slot, source, rows):
        value = source[rows].astype(F32)
        zero = jnp.zeros((rows.stop - rows.start, 1, 256), F32)
        put = slice(1 + rows.start, 1 + rows.stop)
        shifted[slot, 0, put] = jnp.concatenate([zero, value[:, :15]], axis=1).astype(BF16)
        shifted[slot, 1, put] = value.astype(BF16)
        shifted[slot, 2, put] = jnp.concatenate([value[:, 1:], zero], axis=1).astype(BF16)

    for slot in range(3):
        for dx in range(3):
            shifted[slot, dx, 0] = jnp.zeros((16, 256), BF16)
            shifted[slot, dx, 33] = jnp.zeros((16, 256), BF16)

    def taps(slot, dt, first_row, rows):
        total = None
        for dy in range(3):
            for dx in range(3):
                part = jnp.dot(
                    shifted[slot, dx, first_row + dy : first_row + dy + rows].reshape(16 * rows, 256),
                    w[dt, dy, dx], preferred_element_type=F32,
                )
                total = part if total is None else total + part
        return total.reshape(rows, 16, 256)

    frame_loads[1].wait()
    shift(0, feat.at[0], slice(0, 32))
    shift(1, feat.at[1], slice(0, 32))
    loads[1].wait()
    acc[0] = taps(0, 1 - mp, 0, 32) + taps(1, 2 - mp, 0, 32)
    acc[1] = jnp.zeros((32, 16, 256), F32)

    pl.semaphore_wait(met.at[0], 4)
    tell(met.at[1], [(0, 2), (0, -2), (2, 0), (-2, 0)])

    loads[2].wait()
    wl4[...] = jnp.zeros((4, 128, 256), BF16)
    for k in range(4):
        wl4[k, 16 * k : 16 * k + 16] = wl[...]
    loads[3].wait()
    hot = jnp.where(lax.broadcasted_iota(jnp.int32, (256, 256), 0) == order[...], 1.0, 0.0).astype(F32)
    perm_t[...] = hot.astype(BF16)
    perm[...] = hot.T.astype(BF16)

    first = frame == 1
    slot3 = jnp.where(first, 0, 2)
    dt3 = jnp.where(first, 2, 2 * mp)
    dst3 = jnp.where(first, 1, 0)

    def to_tokens(slot, source, h):
        half = slice(16 * h, 16 * h + 16)
        value = source[half].astype(F32) + jax.nn.silu(acc[slot, half])
        for c in range(2):
            act[c] = value[:, :, 128 * c : 128 * c + 128]
        total = None
        for dx in range(2):
            columns = jnp.concatenate(
                [act[c, :, pl.ds(dx, 8, stride=2), :] for c in range(2)], axis=-1
            ).reshape(8, 2, 8, 256)
            for dy in range(2):
                part = lax.dot_general(
                    columns[:, dy].reshape(64, 256).astype(BF16), wl4[2 * dy + dx],
                    (((1,), (1,)), ((), ())), preferred_element_type=F32,
                )
                total = part if total is None else total + part
        tokbuf[slot, 8 * h : 8 * h + 8] = total.reshape(8, 8, 128).astype(BF16)

    def token_copy(slot, to, index):
        band, device = member(index)
        return pltpu.make_async_remote_copy(
            src_ref=tokbuf.at[slot, band], dst_ref=tokin.at[to],
            send_sem=tok_send.at[slot, index], recv_sem=tok_recv.at[to],
            device_id=device, device_id_type=MESH,
        )

    def send_tokens(slot, to, h):
        def step(k, carry):
            index = 16 * h + rem(me + k, 16)

            @pl.when(index != me)
            def _():
                token_copy(slot, to, index).start()

            return carry

        lax.fori_loop(0, 16, step, 0)

    pl.semaphore_wait(met.at[1], 4)
    tell(met.at[2], [(0, 4), (0, -4)])
    for h in range(2):
        for q in (2 * h, 2 * h + 1):
            @pl.when(has_peer)
            def _():
                halo_copies[q].wait_recv()

            @pl.when(jnp.logical_not(has_peer))
            def _():
                halo[parts[q]] = jnp.zeros((parts[q].stop - parts[q].start, 16, 256), BF16)

            shift(2, halo, parts[q])
            acc[dst3, 8 * q : 8 * q + 8] += taps(slot3, dt3, 8 * q, 8)

        @pl.when(mp == 0)
        def _():
            to_tokens(0, feat.at[1], h)

        @pl.when(mp == 1)
        def _():
            to_tokens(0, halo, h)

        @pl.when(frame < FRAMES)
        def _():
            send_tokens(0, frame, h)

        @pl.when(first)
        def _():
            to_tokens(1, feat.at[0], h)
            send_tokens(1, 0, h)

    @pl.when(frame < FRAMES)
    def _():
        tokin[frame] = tokbuf[0, seq]

    @pl.when(first)
    def _():
        tokin[0] = tokbuf[1, seq]

    pl.semaphore_wait(met.at[2], 2)
    tell(met.at[3], [(k, 0) for k in range(1, NY)])

    loads[4].wait()
    for block in range(NZH * NY // 2):
        zh_of, y_of = block // (NY // 2), 2 * (block % (NY // 2))
        moved = jnp.dot(perm_t[...], cot[:, 256 * block : 256 * block + 256], preferred_element_type=F32)
        turned = moved.T.reshape(2, 2, 2, NX, 8, 256)
        for pair in range(2):
            for one in range(2):
                for tx in range(NX):
                    cot_t[2 * zh_of + pair, one, tx, 8 * y_of : 8 * y_of + 16] = jnp.concatenate(
                        [turned[0, pair, one, tx], turned[1, pair, one, tx]], axis=0
                    ).astype(BF16)

    def token_wait(f, carry):
        own = jnp.logical_or(frame == f, jnp.logical_and(first, f == 0))

        @pl.when(jnp.logical_not(own))
        def _():
            pltpu.make_async_remote_copy(
                src_ref=tokbuf.at[0, 0], dst_ref=tokin.at[f],
                send_sem=tok_send.at[0, 0], recv_sem=tok_recv.at[f],
                device_id=partner, device_id_type=MESH,
            ).wait_recv()

        return carry

    lax.fori_loop(0, FRAMES, token_wait, 0)
    tok = tokin[...].astype(F32).reshape(256, 128)
    tok_a = tok.astype(BF16)
    tok_b = jnp.concatenate([tok[:, 64:], tok[:, :64]], axis=1).astype(BF16)

    far_first = (3, 2, 4, 1, 5, 0)
    pair = div(z, 2)

    def x_copy(o, k):
        tx, device = x_peer(k)
        return pltpu.make_async_remote_copy(
            src_ref=gsend.at[o, tx], dst_ref=xrecv.at[o, k - 1],
            send_sem=x_send.at[o, k - 1], recv_sem=x_recv.at[o, k - 1],
            device_id=device, device_id_type=MESH,
        )

    def send_x(o):
        c = rem(pair + far_first[o], NZ // 2)
        gsend[o] = (
            jnp.dot(cot_t[c, 0].reshape(256, 256), tok_a, preferred_element_type=F32)
            + jnp.dot(cot_t[c, 1].reshape(256, 256), tok_b, preferred_element_type=F32)
        ).astype(BF16).reshape(NX, 64, 128)
        for k in (2, 1, 3):
            x_copy(o, k).start()

    for o in range(DEPTH):
        send_x(o)

    loads[5].wait()
    ordered = jnp.dot(perm[...], tok_a, preferred_element_type=F32).astype(BF16)[:, :64]
    for i in range(0, 3072, 512):
        embedded_ref[:, i : i + 512] = jnp.dot(
            ordered, emb[:, i : i + 512], preferred_element_type=F32
        ).astype(BF16)

    def plane_copy(o, one, ky):
        tz = 2 * rem(pair + far_first[o], NZ // 2) + one
        slot = rem(tz - z + NZ, NZ) * NY + ky
        ty = rem(y + ky, NY)
        return slot, pltpu.make_async_remote_copy(
            src_ref=ysend.at[o, ty], dst_ref=yzrecv.at[slot],
            send_sem=yz_send.at[o, one, ky], recv_sem=yz_recv.at[slot],
            device_id=(div(tz, NZL) * NY + ty, rem(tz, NZL) * NX + x, mp), device_id_type=MESH,
        )

    def each_plane_copy(o, act_on):
        for ky in (4, 3, 5, 2, 6, 1, 7, 0):
            for one in range(2):
                slot, copy = plane_copy(o, one, ky)
                if far_first[o] or ky:
                    act_on(copy)
                else:
                    @pl.when(slot != 0)
                    def _():
                        act_on(copy)

    pl.semaphore_wait(met.at[3], NY - 1)
    for o in range(6):
        total = gsend[o, x].astype(F32)
        for k in range(1, NX):
            x_copy(o, k).wait_recv()
            total += xrecv[o, k - 1].astype(F32)
        ysend[o] = total.reshape(NY, 8, 128).astype(BF16)
        each_plane_copy(o, lambda copy: copy.start())

    @pl.when(has_peer)
    def _():
        for copy in halo_copies:
            copy.wait_send()

    def drain(slot, to):
        def step(index, carry):
            @pl.when(index != me)
            def _():
                token_copy(slot, to, index).wait_send()

            return carry

        lax.fori_loop(0, GROUP, step, 0)

    @pl.when(frame < FRAMES)
    def _():
        drain(0, frame)

    @pl.when(first)
    def _():
        drain(1, 0)

    for o in range(6):
        for k in range(1, NX):
            x_copy(o, k).wait_send()
        each_plane_copy(o, lambda copy: copy.wait_send())

    total = ysend[5, y].astype(F32)
    for kz in (0, 1, 11, 2, 10, 3, 9, 4, 8, 5, 7, 6):
        for ky in (0, 1, 7, 2, 6, 3, 5, 4):
            slot = kz * NY + ky
            if slot:
                pltpu.make_async_remote_copy(
                    src_ref=ysend.at[0, 0], dst_ref=yzrecv.at[slot],
                    send_sem=yz_send.at[0, 0, 0], recv_sem=yz_recv.at[slot],
                    device_id=partner, device_id_type=MESH,
                ).wait_recv()
                total += yzrecv[slot].astype(F32)
    grad_ref[...] = jnp.where(rem(z, 2) == 0, total[:, :64], total[:, 64:])


def finish(embedded_ref, partial_ref, embedded_hbm, grad_hbm, sem):
    copies = [pltpu.make_async_copy(partial_ref, grad_hbm, sem.at[8])]
    for i in range(8):
        rows = pl.ds(32 * i, 32)
        copies.append(pltpu.make_async_copy(embedded_ref.at[rows], embedded_hbm.at[rows], sem.at[i]))
    for copy in copies:
        copy.start()
    for copy in copies:
        copy.wait()


def local(features, conv_weight, latent_weight, order, embed_weight, cotangent):
    dma = pltpu.SemaphoreType.DMA
    vmem = pl.BlockSpec(memory_space=pltpu.VMEM)
    embedded, partial = pl.pallas_call(
        kernel,
        name="section",
        out_shape=(
            jax.ShapeDtypeStruct((256, 3072), BF16),
            jax.ShapeDtypeStruct((8, 64), F32),
        ),
        in_specs=[pl.BlockSpec(memory_space=pltpu.HBM)] * 6,
        out_specs=(vmem, vmem),
        scratch_shapes=[
            pltpu.VMEM((2, 32, 16, 256), BF16),
            pltpu.VMEM((3, 3, 3, 256, 256), BF16),
            pltpu.VMEM((16, 256), BF16),
            pltpu.VMEM((1, 256), jnp.int32),
            pltpu.VMEM((256, 3072), BF16),
            pltpu.VMEM((64, 3072), BF16),
            pltpu.VMEM((32, 16, 256), BF16),
            pltpu.VMEM((3, 3, 34, 16, 256), BF16),
            pltpu.VMEM((2, 32, 16, 256), F32),
            pltpu.VMEM((2, 16, 16, 128), F32),
            pltpu.VMEM((4, 128, 256), BF16),
            pltpu.VMEM((256, 256), BF16),
            pltpu.VMEM((256, 256), BF16),
            pltpu.VMEM((6, 2, NX, 64, 256), BF16),
            pltpu.VMEM((2, 16, 8, 128), BF16),
            pltpu.VMEM((32, 8, 128), BF16),
            pltpu.VMEM((6, NX, 64, 128), BF16),
            pltpu.VMEM((6, NX - 1, 64, 128), BF16),
            pltpu.VMEM((6, NY, 8, 128), BF16),
            pltpu.VMEM((NZ * NY, 8, 128), BF16),
            dma((8,)),
            dma((4,)), dma((4,)),
            dma((2, GROUP)), dma((FRAMES,)),
            dma((6, NX - 1)), dma((6, NX - 1)),
            dma((6, 2, NY)), dma((NZ * NY,)),
            pltpu.SemaphoreType.REGULAR((4,)),
        ],
        compiler_params=pltpu.CompilerParams(
            collective_id=0, has_side_effects=True, vmem_limit_bytes=32 * 1024 * 1024
        ),
    )(
        *(
            pltpu.with_memory_space_constraint(value, pltpu.HBM)
            for value in (features, conv_weight, latent_weight.T, order.reshape(1, 256), cotangent, embed_weight)
        )
    )
    embedded, grad = pl.pallas_call(
        finish,
        name="finish",
        out_shape=(
            jax.ShapeDtypeStruct((256, 3072), BF16),
            jax.ShapeDtypeStruct((8, 64), F32),
        ),
        in_specs=[vmem] * 2,
        out_specs=(pl.BlockSpec(memory_space=pltpu.HBM),) * 2,
        scratch_shapes=[dma((9,))],
        compiler_params=pltpu.CompilerParams(vmem_limit_bytes=16 * 1024 * 1024),
    )(embedded, partial)
    return embedded, grad.T[None]


def solution(mesh):
    placed = (
        P("dp", "seq", None, None, None),
        P(),
        P(),
        P(),
        P(None, "mp"),
        P(("dp", "seq"), "mp"),
    )
    return jax.shard_map(
        local,
        mesh=mesh,
        in_specs=placed,
        out_specs=(P(("dp", "seq"), "mp"), P("mp", None, ("dp", "seq"))),
        check_vma=False,
    )
```
